32 devices in a mesh: rows: 16 (over z, y, x), inner: 2 (over core).
Axes of the slice: x: 2, y: 2, z: 4, core: 2. Of those that a mesh axis runs over, the one named last changes fastest.
Arguments:
- r_tiles: bfloat16 [128, 16, 128, 128], P('rows', 'inner'), may hold values from -0.5 to 0.5
- r_cols: int32 [128, 16], P('rows', 'inner'), may hold values from 0 to 255, as said below
- a_tiles: bfloat16 [256, 7, 128, 128], P(('rows', 'inner')), may hold values from -6 to 6
- a_cols: int32 [256, 7], replicated, may hold values from 0 to 255, as said below
- c_cols: int32 [128, 8], P('rows'), may hold values from -1 to 255, as said below
- c_counts: int32 [128], P('rows'), may hold values from 4 to 8, as said below
Outputs:
- c_tiles: bfloat16 [128, 8, 128, 128], P('rows', 'inner')
- row_offsets: int32 [128], P('rows')
The draws below stay inside these ranges and needn't reach their ends.
Inputs may be any that keep to these rules, and one draw needn't show every extreme that they name: `r_cols`: the slots g * 8 to (g + 1) * 8 - 1 of block row c name distinct fine block rows k with (k // 8) % 2 == g and k // 16 within one of c // 8. `a_cols`: row k names 7 distinct fine block columns, the first of them k. `c_cols`: the first c_counts[c] entries of row c are distinct block columns, the others are -1. `c_counts`: each aligned group of 8 block rows has one with 8 live slots.
All inputs are finite; a program needn't handle non-finite values.
Results may differ from the reference program's by a relative error of at most 0.001.
Values may be sent and summed in bfloat16 or wider, within the bound.
A program may use at most 64 MiB of HBM per device.

```python
import jax
import jax.numpy as jnp
from jax import lax

TB = 128
RB_DEV = 8
SR_DEV = 8
KA_DEV = 8
SA = 7
CAP = 8
NCB = 128
SR = 16
NK = 256
N_ROWS = 16
N_INNER = 2


def pattern(key):
    span = 3 * KA_DEV
    coarse_owner = jnp.arange(NCB, dtype=jnp.int32) // RB_DEV
    candidate = jnp.arange(span, dtype=jnp.int32)
    shift_rows = candidate // KA_DEV - 1
    neighbour = coarse_owner[:, None, None] + shift_rows[None, None, :]
    usable = (neighbour >= 0) & (neighbour < N_ROWS)
    group_ids = jnp.arange(N_INNER, dtype=jnp.int32)
    noise_r = jax.random.randint(jax.random.fold_in(key, 101), (NCB, N_INNER, span), 0, 65536)
    scores = noise_r * span + candidate[None, None, :]
    scores = jnp.where((candidate == 0)[None, None, :] & usable, -2, scores)
    scores = jnp.where((candidate == 2 * KA_DEV)[None, None, :] & usable, -1, scores)
    scores = jnp.where(usable, scores, 2 ** 30)
    chosen_q = jnp.argsort(scores, axis=-1)[:, :, :SR_DEV].astype(jnp.int32)
    chosen_shift = chosen_q // KA_DEV - 1
    chosen_local = chosen_q % KA_DEV
    fine_rows = ((coarse_owner[:, None, None] + chosen_shift) * N_INNER + group_ids[None, :, None]) * KA_DEV + chosen_local
    r_columns = fine_rows.reshape(NCB, SR).astype(jnp.int32)
    first_stride = jax.random.randint(jax.random.fold_in(key, 606), (), 9, 17).astype(jnp.int32)
    second_raw = jax.random.randint(jax.random.fold_in(key, 707), (), 9, 17).astype(jnp.int32)
    second_stride = jnp.clip(second_raw, 2, (NK // 2 - 1) // first_stride)
    plane_stride = first_stride * second_stride
    stencil = jnp.stack([jnp.int32(1), jnp.int32(-1), first_stride, -first_stride, plane_stride, -plane_stride]).astype(jnp.int32)
    noise_a = jax.random.randint(jax.random.fold_in(key, 202), (NK, 6), 0, 65536)
    order_ids = jnp.argsort(noise_a * 6 + jnp.arange(6, dtype=jnp.int32)[None, :], axis=-1)[:, :SA - 1]
    fine_ids = jnp.arange(NK, dtype=jnp.int32)
    others = jnp.mod(fine_ids[:, None] + stencil[order_ids], NK)
    a_columns = jnp.concatenate([fine_ids[:, None], others], axis=1).astype(jnp.int32)
    base_counts = jax.random.randint(jax.random.fold_in(key, 303), (NCB,), CAP // 2, CAP + 1)
    full_at = jax.random.randint(jax.random.fold_in(key, 404), (N_ROWS,), 0, RB_DEV)
    is_full = jnp.arange(NCB, dtype=jnp.int32) % RB_DEV == jnp.repeat(full_at, RB_DEV)
    counts = jnp.where(is_full, CAP, base_counts).astype(jnp.int32)
    product_columns = a_columns[r_columns]
    slot_ids = jnp.arange(SR, dtype=jnp.int32)
    favoured = ((slot_ids // SR_DEV)[None, :] == (jnp.arange(NCB, dtype=jnp.int32) % N_INNER)[:, None]) & (slot_ids % SR_DEV < 2)[None, :]
    favoured = favoured[:, :, None] & (jnp.arange(SA, dtype=jnp.int32) == 0)[None, None, :]
    noise_c = jax.random.randint(jax.random.fold_in(key, 505), (NCB, SR, SA), 0, 4096)
    weights = jnp.where(favoured, 0, noise_c + 1)
    packed = (product_columns * 8192 + weights).reshape(NCB, SR * SA)
    ordered = jnp.sort(packed, axis=-1)
    values = ordered // 8192
    ranks = ordered % 8192
    leading = jnp.concatenate([jnp.ones((NCB, 1), dtype=bool), values[:, 1:] != values[:, :-1]], axis=1)
    select_key = jnp.where(leading, ranks * (SR * SA) + jnp.arange(SR * SA, dtype=jnp.int32)[None, :], 2 ** 30)
    selected = jnp.argsort(select_key, axis=-1)[:, :CAP]
    taken = jnp.take_along_axis(values, selected, axis=1)
    c_columns = jnp.where(jnp.arange(CAP, dtype=jnp.int32)[None, :] < counts[:, None], taken, -1).astype(jnp.int32)
    return (r_columns, a_columns, c_columns, counts)


def draw_r_cols(key, part):
    return pattern(key)[0]


def draw_a_cols(key, part):
    return pattern(key)[1]


def draw_c_cols(key, part):
    return pattern(key)[2]


def draw_c_counts(key, part):
    return pattern(key)[3]


def block_levels(own_key, dims, split, smallest, top_value):
    factor_of = 1.0
    for position, parts in split:
        steps = jax.random.uniform(jax.random.fold_in(jax.random.fold_in(own_key, 6), position), (parts,), jnp.float32, smallest / len(split), top_value / len(split))
        factor_of = factor_of * jnp.repeat(jnp.exp(steps), dims[position] // parts).reshape((-1,) + (1,) * (len(dims) - 1 - position))
    return factor_of


def scatter_about(rng, dims, spread, most, split=(), kind=jnp.bfloat16):
    loudness = block_levels(rng, dims, split, -0.22, 0.18) if split else 1.0
    drawn = jax.random.normal(rng, dims, jnp.float32) * spread * loudness
    return jnp.minimum(jnp.maximum(drawn, -most), most).astype(kind)


def setup_inputs(seed: int = 0) -> dict:
    streams_of = jax.random.split(jax.random.key(seed), 7)
    r_tiles = scatter_about(streams_of[0], (NCB, SR, TB, TB), TB ** -0.5, 0.5, ((0, 16), (1, 2)))
    r_cols = draw_r_cols(jax.random.fold_in(streams_of[6], 71), 0)
    a_tiles = scatter_about(streams_of[2], (NK, SA, TB, TB), 1.0, 6.0, ((0, 32),))
    a_cols = draw_a_cols(jax.random.fold_in(streams_of[6], 71), 0)
    c_cols = draw_c_cols(jax.random.fold_in(streams_of[6], 71), 0)
    c_counts = draw_c_counts(jax.random.fold_in(streams_of[6], 71), 0)
    return dict(r_tiles=r_tiles, r_cols=r_cols, a_tiles=a_tiles, a_cols=a_cols, c_cols=c_cols, c_counts=c_counts)


def reference(r_tiles, r_cols, a_tiles, a_cols, c_cols, c_counts):
    def one_row(row_data):
        row_tiles, columns, wanted = row_data
        picked = a_tiles[columns].astype(jnp.float32)
        products = jnp.einsum("jxy,jtyz->jtxz", row_tiles.astype(jnp.float32), picked, precision=lax.Precision.HIGHEST)
        matches = (wanted[:, None, None] == a_cols[columns][None]).astype(jnp.float32)
        summed = jnp.einsum("sjt,jtxz->sxz", matches, products, precision=lax.Precision.HIGHEST)
        return summed.astype(jnp.bfloat16)

    c_tiles = lax.map(one_row, (r_tiles, r_cols, c_cols))
    row_offsets = (jnp.cumsum(c_counts) - c_counts).astype(jnp.int32)
    return c_tiles, row_offsets
```

```python
import functools

import jax
import jax.numpy as jnp
from jax import lax
from jax.experimental import pallas as pl
from jax.experimental.pallas import tpu as pltpu
from jax.sharding import PartitionSpec as P

MESH = pl.DeviceIdType.MESH
BATCH = 4


def plan_kernel(dims, meta_ref, near_ref, own_ref, code_ref, plan_ref, gathered, send_sem, recv_sem):
    rows, groups, local_rows, op_slots, r_slots, cap, half = dims
    width = 2 * half
    count = rows * groups
    tiles = local_rows * op_slots
    row = lax.axis_index("rows")
    group = lax.axis_index("inner")
    me = row * groups + group

    barrier = pltpu.get_barrier_semaphore()

    def place(step):
        other = lax.rem(me + step, count)
        return (other // groups, lax.rem(other, groups))

    def greet(step, carry):
        pl.semaphore_signal(barrier, inc=1, device_id=place(step), device_id_type=MESH)
        return carry

    lax.fori_loop(1, count, greet, 0)
    gathered[me] = meta_ref[...]
    pl.semaphore_wait(barrier, count - 1)

    def post(step, carry):
        pltpu.make_async_remote_copy(
            src_ref=meta_ref,
            dst_ref=gathered.at[me],
            send_sem=send_sem,
            recv_sem=recv_sem,
            device_id=place(step),
            device_id_type=MESH,
        ).start()
        return carry

    lax.fori_loop(1, count, post, 0)
    everyone = gathered.at[pl.ds(0, count - 1)]
    pltpu.make_async_copy(everyone, everyone, send_sem).wait()
    pltpu.make_async_copy(everyone, everyone, recv_sem).wait()

    row_count = meta_ref.shape[0]
    lanes = lax.broadcasted_iota(jnp.int32, (row_count, width), 1)

    def matches(block, columns, fine_rows):
        named = fine_rows == block[:, 0:1]
        for j in range(1, r_slots):
            named = named | (fine_rows == block[:, j : j + 1])
        slot = jnp.full((row_count, width), -1, jnp.int32)
        for s in range(cap):
            slot = jnp.where(columns == block[:, r_slots + s : r_slots + s + 1], s, slot)
        return jnp.where(named, slot, -1)

    def near_rows(device):
        owner = device // groups
        kind = lax.rem(device, groups)
        step = jnp.where(lanes < half, -1, 1)
        tile = jnp.where(lanes < half, lanes, lanes - half)
        inside = tile < tiles
        fine = ((owner + step) * groups + kind) * local_rows + tile // op_slots
        return jnp.where(inside, fine, -5)

    def near_matches(device):
        return matches(gathered[device], near_ref[pl.ds(device, 1), :], near_rows(device))

    def wanted(found):
        return jnp.max((found >= 0).astype(jnp.int32), axis=0, keepdims=True)

    def widest(device, most):
        need = wanted(near_matches(device))
        low = jnp.sum(jnp.where(lanes[0:1] < half, need, 0), axis=1, keepdims=True)
        high = jnp.sum(jnp.where(lanes[0:1] < half, 0, need), axis=1, keepdims=True)
        return jnp.maximum(most, jnp.maximum(low, high))

    most = lax.fori_loop(0, count, widest, jnp.zeros((1, 1), jnp.int32), unroll=2)

    down = lax.broadcasted_iota(jnp.int32, (width, width), 0)
    across = lax.broadcasted_iota(jnp.int32, (width, width), 1)
    same = (down < half) == (across < half)

    def ranks(need):
        spread = jnp.broadcast_to(need, (width, width))
        column = jnp.sum(jnp.where(down == across, spread, 0), axis=1, keepdims=True)
        before = jnp.sum(jnp.where((across < down) & same, spread, 0), axis=1, keepdims=True)
        along = jnp.sum(
            jnp.where((down < across) & same, jnp.broadcast_to(column, (width, width)), 0),
            axis=0,
            keepdims=True,
        )
        return column, before, along

    def send_list(device, high):
        column, before, _ = ranks(wanted(near_matches(device)))
        first = half if high else 0
        mine = (down >= half) if high else (down < half)
        chosen = mine & (column > 0) & (before == across)
        return jnp.sum(jnp.where(chosen, down - first, 0), axis=0, keepdims=True)

    left = jnp.maximum(row - 1, 0) * groups + group
    right = jnp.minimum(row + 1, rows - 1) * groups + group
    plan_ref[0:1, :] = send_list(left, True)
    plan_ref[1:2, :] = send_list(right, False)

    found = near_matches(me)
    _, _, along = ranks(wanted(found))
    slot_at = along + jnp.where(lanes[0:1] < half, tiles, 2 * tiles)
    code_ref[:, 0:width] = jnp.where(found >= 0, found + cap * slot_at, -1)
    fine = me * local_rows + jnp.where(lanes < tiles, lanes // op_slots, 0)
    fine = jnp.where(lanes < tiles, fine, -5)
    found = matches(gathered[me], own_ref[pl.ds(me, 1), :], fine)
    code_ref[:, width:] = jnp.where(found >= 0, found + cap * lanes, -1)

    live = r_slots + cap

    def earlier(index, total):
        block = gathered[index * groups]
        return total + jnp.sum(block[:, live : live + 1], axis=0, keepdims=True)

    first = lax.fori_loop(0, row, earlier, jnp.zeros((1, 1), jnp.int32))
    counts = jnp.broadcast_to(gathered[me][:, live : live + 1], (row_count, width))
    above = lax.broadcasted_iota(jnp.int32, (row_count, width), 0)
    inner_sum = jnp.sum(jnp.where(above < lanes, counts, 0), axis=0, keepdims=True)
    plan_ref[2:3, :] = inner_sum + first
    plan_ref[3:4, :] = jnp.broadcast_to(most, (1, width))


def halo_kernel(rows, size, plan_ref, a_ref, out_ref, packed, send_sems, recv_sems):
    row = lax.axis_index("rows")
    group = lax.axis_index("inner")
    barrier = pltpu.get_barrier_semaphore()
    has_left = row > 0
    has_right = row < rows - 1

    @pl.when(has_left)
    def _():
        pl.semaphore_signal(barrier, inc=1, device_id=(row - 1, group), device_id_type=MESH)

    @pl.when(has_right)
    def _():
        pl.semaphore_signal(barrier, inc=1, device_id=(row + 1, group), device_id_type=MESH)

    def pack(index, carry):
        packed[0, index] = a_ref[plan_ref[0, index]]
        packed[1, index] = a_ref[plan_ref[1, index]]
        return carry

    lax.fori_loop(0, size, pack, 0, unroll=2)

    pl.semaphore_wait(barrier, has_left.astype(jnp.int32) + has_right.astype(jnp.int32))

    def copy(side, other):
        return pltpu.make_async_remote_copy(
            src_ref=packed.at[side],
            dst_ref=out_ref.at[1 - side, pl.ds(0, size)],
            send_sem=send_sems.at[side],
            recv_sem=recv_sems.at[1 - side],
            device_id=(other, group),
            device_id_type=MESH,
        )

    @pl.when(has_left)
    def _():
        copy(0, row - 1).start()

    @pl.when(has_right)
    def _():
        copy(1, row + 1).start()

    @pl.when(has_left)
    def _():
        copy(0, row - 1).wait_send()
        copy(1, row - 1).wait_recv()

    @pl.when(has_right)
    def _():
        copy(1, row + 1).wait_send()
        copy(0, row + 1).wait_recv()


def product_kernel(dims, code_ref, cols_ref, r_ref, a_ref, halo_ref, out_ref, tiles_ref, job_r, job_a, job_c, sems):
    rows, groups, local_rows, op_slots, r_slots, cap, half = dims
    width = 2 * half
    tiles = local_rows * op_slots
    row_count = cols_ref.shape[0]
    own_cap = cap // groups
    row = lax.axis_index("rows")
    group = lax.axis_index("inner")
    own = pltpu.make_async_copy(a_ref, tiles_ref.at[pl.ds(0, tiles)], sems.at[0])
    near = pltpu.make_async_copy(halo_ref, tiles_ref.at[pl.ds(tiles, 2 * tiles)], sems.at[1])
    own.start()
    near.start()
    last = groups * row_count * own_cap

    def clear(index, carry):
        out_ref[index] = jnp.zeros(out_ref.shape[1:], jnp.float32)
        return carry

    lax.fori_loop(0, last, clear, 0, unroll=4)

    def list_row(c, found):
        def list_slot(j, found):
            fine = cols_ref[c, j]
            side = fine // (local_rows * groups) - row
            base = jnp.where(side == 0, width, jnp.where(side < 0, 0, half))
            base = base + lax.rem(fine, local_rows) * op_slots
            for t in range(op_slots):
                code = code_ref[c, base + t]
                slot = lax.rem(code, cap)
                ahead = lax.rem(slot // own_cap + groups - group, groups)
                job_r[found] = c * r_slots + j
                job_a[found] = code // cap
                job_c[found] = (ahead * row_count + c) * own_cap + lax.rem(slot, own_cap)
                found = found + (code >= 0).astype(jnp.int32)
            return found

        return lax.fori_loop(0, r_slots, list_slot, found)

    found = lax.fori_loop(0, row_count, list_row, jnp.int32(0))
    for extra in range(BATCH):
        job_r[found + extra] = 0
        job_a[found + extra] = 0
        job_c[found + extra] = last
    own.wait()
    near.wait()

    def batch(step, carry):
        results = []
        for extra in range(BATCH):
            index = step * BATCH + extra
            results.append(
                jnp.dot(
                    r_ref[job_r[index]],
                    tiles_ref[job_a[index]],
                    preferred_element_type=jnp.float32,
                )
            )
        for extra in range(BATCH):
            target = job_c[step * BATCH + extra]
            out_ref[target] = out_ref[target] + results[extra]
        return carry

    lax.fori_loop(0, (found + BATCH - 1) // BATCH, batch, 0)


def sum_kernel(groups, pieces, part_ref, out_ref, landed, send_sems, recv_sems):
    row = lax.axis_index("rows")
    group = lax.axis_index("inner")
    own = out_ref.shape[0]
    piece = own // pieces
    barrier = pltpu.get_barrier_semaphore()
    for ahead in range(1, groups):
        pl.semaphore_signal(
            barrier, inc=1, device_id=(row, lax.rem(group + ahead, groups)), device_id_type=MESH
        )
    pl.semaphore_wait(barrier, groups - 1)
    copies = []
    for ahead in range(1, groups):
        for part in range(pieces):
            copy = pltpu.make_async_remote_copy(
                src_ref=part_ref.at[pl.ds(ahead * own + part * piece, piece)],
                dst_ref=landed.at[ahead - 1, pl.ds(part * piece, piece)],
                send_sem=send_sems.at[ahead - 1, part],
                recv_sem=recv_sems.at[ahead - 1, part],
                device_id=(row, lax.rem(group + ahead, groups)),
                device_id_type=MESH,
            )
            copy.start()
            copies.append(copy)
    for part in range(pieces):
        for ahead in range(1, groups):
            copies[(ahead - 1) * pieces + part].wait_recv()

        def add(index, carry):
            total = part_ref[index]
            for ahead in range(1, groups):
                total = total + landed[ahead - 1, index]
            out_ref[index] = total.astype(out_ref.dtype)
            return carry

        lax.fori_loop(part * piece, (part + 1) * piece, add, 0)
    for copy in copies:
        copy.wait_send()


def sizes_for(tiles):
    steps = [8, 12, 16, 18, 20, 22, 24, 26, 28, 30, 32, 36, 40, 48]
    return [size for size in steps if size < tiles] + [tiles]


def body(rows, groups, r_tiles, r_cols, a_tiles, a_cols, c_cols, c_counts):
    local_rows, op_slots, tile, _ = a_tiles.shape
    row_count, r_slots = r_tiles.shape[:2]
    cap = c_cols.shape[1]
    tiles = local_rows * op_slots
    half = -(-tiles // 64) * 64
    width = 2 * half
    count = rows * groups
    own_cap = cap // groups
    dims = (rows, groups, local_rows, op_slots, r_slots, cap, half)
    vmem = pl.BlockSpec(memory_space=pltpu.VMEM)
    smem = pl.BlockSpec(memory_space=pltpu.SMEM)
    anywhere = pl.BlockSpec(memory_space=pl.ANY)

    meta = jnp.concatenate([r_cols, c_cols, c_counts[:, None]], axis=1)
    meta = jnp.pad(meta, ((0, 0), (0, width - meta.shape[1])), constant_values=-9)
    flat = a_cols.reshape(count, tiles)
    narrow = jnp.pad(flat, ((groups, groups), (0, half - tiles)), constant_values=-2)
    near = jnp.concatenate([narrow[:count], narrow[2 * groups :]], axis=1)
    own = jnp.pad(flat, ((0, 0), (0, width - tiles)), constant_values=-2)

    code, plan = pl.pallas_call(
        functools.partial(plan_kernel, dims),
        out_shape=(
            jax.ShapeDtypeStruct((row_count, 2 * width), jnp.int32),
            jax.ShapeDtypeStruct((8, width), jnp.int32),
        ),
        in_specs=[vmem] * 3,
        out_specs=(vmem, vmem),
        scratch_shapes=[
            pltpu.VMEM((count, row_count, width), jnp.int32),
            pltpu.SemaphoreType.DMA,
            pltpu.SemaphoreType.DMA,
        ],
        compiler_params=pltpu.CompilerParams(collective_id=0, has_side_effects=True),
        name="plan",
    )(meta, near, own)

    flat_a = a_tiles.reshape(tiles, tile, tile)
    sizes = sizes_for(tiles)

    def exchange(number, size, plan, flat_a):
        return pl.pallas_call(
            functools.partial(halo_kernel, rows, size),
            out_shape=jax.ShapeDtypeStruct((2, tiles, tile, tile), a_tiles.dtype),
            in_specs=[smem, vmem],
            out_specs=anywhere,
            scratch_shapes=[
                pltpu.VMEM((2, size, tile, tile), a_tiles.dtype),
                pltpu.SemaphoreType.DMA((2,)),
                pltpu.SemaphoreType.DMA((2,)),
            ],
            compiler_params=pltpu.CompilerParams(collective_id=number + 2, has_side_effects=True),
            name=f"halo{size}",
        )(plan, flat_a)

    level = jnp.sum((plan[3, 0] > jnp.array(sizes[:-1], jnp.int32)).astype(jnp.int32))
    halo = lax.switch(
        level,
        [functools.partial(exchange, number, size) for number, size in enumerate(sizes)],
        plan,
        flat_a,
    )

    slots = row_count * r_slots * op_slots + BATCH
    partial_value = pl.pallas_call(
        functools.partial(product_kernel, dims),
        out_shape=jax.ShapeDtypeStruct((row_count * cap + 1, tile, tile), jnp.float32),
        in_specs=[smem, smem, vmem, anywhere, anywhere],
        out_specs=vmem,
        scratch_shapes=[
            pltpu.VMEM((3 * tiles, tile, tile), a_tiles.dtype),
            pltpu.SMEM((slots,), jnp.int32),
            pltpu.SMEM((slots,), jnp.int32),
            pltpu.SMEM((slots,), jnp.int32),
            pltpu.SemaphoreType.DMA((2,)),
        ],
        name="products",
    )(
        code,
        r_cols,
        r_tiles.reshape(row_count * r_slots, tile, tile),
        flat_a,
        halo.reshape(2 * tiles, tile, tile),
    )

    own_count = row_count * own_cap
    pieces = 4 if own_count % 4 == 0 else 1
    c_tiles = pl.pallas_call(
        functools.partial(sum_kernel, groups, pieces),
        out_shape=jax.ShapeDtypeStruct((own_count, tile, tile), jnp.bfloat16),
        in_specs=[vmem],
        out_specs=vmem,
        scratch_shapes=[
            pltpu.VMEM((groups - 1, own_count, tile, tile), jnp.float32),
            pltpu.SemaphoreType.DMA((groups - 1, pieces)),
            pltpu.SemaphoreType.DMA((groups - 1, pieces)),
        ],
        compiler_params=pltpu.CompilerParams(collective_id=1, has_side_effects=True),
        name="sums",
    )(partial_value)
    return (c_tiles.reshape(row_count, own_cap, tile, tile), plan[2, :row_count])


def solution(mesh):
    rows = mesh.shape["rows"]
    groups = mesh.shape["inner"]
    return jax.shard_map(
        functools.partial(body, rows, groups),
        mesh=mesh,
        in_specs=(
            P("rows", "inner", None, None),
            P("rows", "inner"),
            P(("rows", "inner"), None, None, None),
            P(),
            P("rows", None),
            P("rows"),
        ),
        out_specs=(P("rows", "inner", None, None), P("rows")),
        check_vma=False,
    )
```

```python
import functools

import jax
import jax.numpy as jnp
from jax import lax
from jax.experimental import pallas as pl
from jax.experimental.pallas import tpu as pltpu
from jax.sharding import PartitionSpec as P

MESH = pl.DeviceIdType.MESH
BATCH = 4


def plan_kernel(
    dims, r_cols_ref, c_cols_ref, counts_ref, columns_ref, code_ref, plan_ref,
    meta_ref, gathered, needs, send_sem, recv_sem,
):
    rows, groups, local_rows, op_slots, r_slots, cap, half = dims
    width = 2 * half
    count = rows * groups
    tiles = local_rows * op_slots
    row = lax.axis_index("rows")
    group = lax.axis_index("inner")
    me = row * groups + group

    barrier = pltpu.get_barrier_semaphore()

    def place(step):
        other = lax.rem(me + step, count)
        return (other // groups, lax.rem(other, groups))

    def greet(step, carry):
        pl.semaphore_signal(barrier, inc=1, device_id=place(step), device_id_type=MESH)
        return carry

    lax.fori_loop(1, count, greet, 0)
    row_count = r_cols_ref.shape[0]
    live = r_slots + cap
    lanes = lax.broadcasted_iota(jnp.int32, (row_count, width), 1)
    above = lax.broadcasted_iota(jnp.int32, (row_count, width), 0)
    small = (row_count, row_count)
    diagonal = lax.broadcasted_iota(jnp.int32, small, 0) == lax.broadcasted_iota(jnp.int32, small, 1)
    spread_counts = jnp.broadcast_to(counts_ref[...], small)
    own_counts = jnp.sum(jnp.where(diagonal, spread_counts, 0), axis=1, keepdims=True)
    meta_ref[...] = jnp.full(meta_ref.shape, -9, jnp.int32)
    meta_ref[:, 0:r_slots] = r_cols_ref[...]
    meta_ref[:, r_slots:live] = c_cols_ref[...]
    meta_ref[:, live : live + 1] = own_counts
    gathered[me] = meta_ref[...]
    pl.semaphore_wait(barrier, count - 1)

    def post(step, carry):
        pltpu.make_async_remote_copy(
            src_ref=meta_ref,
            dst_ref=gathered.at[me],
            send_sem=send_sem,
            recv_sem=recv_sem,
            device_id=place(step),
            device_id_type=MESH,
        ).start()
        return carry

    lax.fori_loop(1, count, post, 0)
    everyone = gathered.at[pl.ds(0, count - 1)]
    pltpu.make_async_copy(everyone, everyone, send_sem).wait()
    pltpu.make_async_copy(everyone, everyone, recv_sem).wait()

    def matches(block, columns, fine_rows):
        named = fine_rows == block[:, 0:1]
        for j in range(1, r_slots):
            named = named | (fine_rows == block[:, j : j + 1])
        slot = jnp.full((row_count, width), -1, jnp.int32)
        for s in range(cap):
            slot = jnp.where(columns == block[:, r_slots + s : r_slots + s + 1], s, slot)
        return jnp.where(named, slot, -1)

    shift = jnp.where(lanes < half, -groups, groups) * local_rows
    tile = jnp.where(lanes < half, lanes, lanes - half)
    lane_rows = jnp.where(tile < tiles, shift + tile // op_slots, -(1 << 24))
    low_lanes = lanes[0:1] < half

    def near_matches(device):
        before = columns_ref[pl.ds(jnp.maximum(device - groups, 0), 1), :]
        after = columns_ref[pl.ds(jnp.minimum(device + groups, count - 1), 1), :]
        columns = jnp.where(low_lanes, before, after)
        return matches(gathered[device], columns, lane_rows + device * local_rows)

    def wanted(found):
        return jnp.max((found >= 0).astype(jnp.int32), axis=0, keepdims=True)

    def gather_needs(device, carry):
        needs[pl.ds(device, 1), :] = wanted(near_matches(device))
        return carry

    lax.fori_loop(0, count, gather_needs, 0, unroll=4)
    every = needs[...]
    low_side = lax.broadcasted_iota(jnp.int32, every.shape, 1) < half
    low = jnp.sum(jnp.where(low_side, every, 0), axis=1, keepdims=True)
    high = jnp.sum(jnp.where(low_side, 0, every), axis=1, keepdims=True)
    most = jnp.max(jnp.maximum(low, high), axis=0, keepdims=True)

    down = lax.broadcasted_iota(jnp.int32, (width, width), 0)
    across = lax.broadcasted_iota(jnp.int32, (width, width), 1)
    same = (down < half) == (across < half)

    def ranks(need):
        spread = jnp.broadcast_to(need, (width, width))
        column = jnp.sum(jnp.where(down == across, spread, 0), axis=1, keepdims=True)
        before = jnp.sum(jnp.where((across < down) & same, spread, 0), axis=1, keepdims=True)
        along = jnp.sum(
            jnp.where((down < across) & same, jnp.broadcast_to(column, (width, width)), 0),
            axis=0,
            keepdims=True,
        )
        return column, before, along

    def send_list(device, high):
        column, before, _ = ranks(needs[pl.ds(device, 1), :])
        first = half if high else 0
        mine = (down >= half) if high else (down < half)
        chosen = mine & (column > 0) & (before == across)
        return jnp.sum(jnp.where(chosen, down - first, 0), axis=0, keepdims=True)

    left = jnp.maximum(row - 1, 0) * groups + group
    right = jnp.minimum(row + 1, rows - 1) * groups + group
    plan_ref[0:1, :] = send_list(left, True)
    plan_ref[1:2, :] = send_list(right, False)

    found = near_matches(me)
    _, _, along = ranks(wanted(found))
    slot_at = along + jnp.where(lanes[0:1] < half, tiles, 2 * tiles)
    code_ref[:, 0:width] = jnp.where(found >= 0, found + cap * slot_at, -1)
    fine = me * local_rows + jnp.where(lanes < tiles, lanes // op_slots, 0)
    fine = jnp.where(lanes < tiles, fine, -5)
    found = matches(gathered[me], columns_ref[pl.ds(me, 1), :], fine)
    code_ref[:, width:] = jnp.where(found >= 0, found + cap * lanes, -1)

    def earlier(index, total):
        block = gathered[index * groups]
        return total + jnp.sum(block[:, live : live + 1], axis=0, keepdims=True)

    first = lax.fori_loop(0, row, earlier, jnp.zeros((1, 1), jnp.int32))
    counts = jnp.broadcast_to(own_counts, (row_count, width))
    inner_sum = jnp.sum(jnp.where(above < lanes, counts, 0), axis=0, keepdims=True)
    plan_ref[2:3, :] = inner_sum + first
    plan_ref[3:4, :] = jnp.broadcast_to(most, (1, width))


def halo_kernel(rows, size, plan_ref, a_ref, out_ref, packed, send_sems, recv_sems):
    row = lax.axis_index("rows")
    group = lax.axis_index("inner")
    barrier = pltpu.get_barrier_semaphore()
    has_left = row > 0
    has_right = row < rows - 1

    @pl.when(has_left)
    def _():
        pl.semaphore_signal(barrier, inc=1, device_id=(row - 1, group), device_id_type=MESH)

    @pl.when(has_right)
    def _():
        pl.semaphore_signal(barrier, inc=1, device_id=(row + 1, group), device_id_type=MESH)

    def pack(index, carry):
        packed[0, index] = a_ref[plan_ref[0, index]]
        packed[1, index] = a_ref[plan_ref[1, index]]
        return carry

    lax.fori_loop(0, size, pack, 0, unroll=2)

    pl.semaphore_wait(barrier, has_left.astype(jnp.int32) + has_right.astype(jnp.int32))

    def copy(side, other):
        return pltpu.make_async_remote_copy(
            src_ref=packed.at[side],
            dst_ref=out_ref.at[1 - side, pl.ds(0, size)],
            send_sem=send_sems.at[side],
            recv_sem=recv_sems.at[1 - side],
            device_id=(other, group),
            device_id_type=MESH,
        )

    @pl.when(has_left)
    def _():
        copy(0, row - 1).start()

    @pl.when(has_right)
    def _():
        copy(1, row + 1).start()

    @pl.when(has_left)
    def _():
        copy(0, row - 1).wait_send()
        copy(1, row - 1).wait_recv()

    @pl.when(has_right)
    def _():
        copy(1, row + 1).wait_send()
        copy(0, row + 1).wait_recv()


def product_kernel(dims, code_ref, cols_ref, r_ref, a_ref, halo_ref, out_ref, tiles_ref, jobs, sems):
    rows, groups, local_rows, op_slots, r_slots, cap, half = dims
    width = 2 * half
    tiles = local_rows * op_slots
    row_count = cols_ref.shape[0]
    own_cap = cap // groups
    row = lax.axis_index("rows")
    group = lax.axis_index("inner")
    own = pltpu.make_async_copy(a_ref, tiles_ref.at[pl.ds(0, tiles)], sems.at[0])
    near = pltpu.make_async_copy(halo_ref, tiles_ref.at[pl.ds(tiles, 2 * tiles)], sems.at[1])
    own.start()
    near.start()
    last = groups * row_count * own_cap
    scale = 1 << (3 * tiles * cap - 1).bit_length()

    def clear(index, carry):
        out_ref[index] = jnp.zeros(out_ref.shape[1:], jnp.float32)
        return carry

    lax.fori_loop(0, last, clear, 0, unroll=4)

    def list_row(c, found):
        def list_slot(j, found):
            fine = cols_ref[c, j]
            side = fine // (local_rows * groups) - row
            base = jnp.where(side == 0, width, jnp.where(side < 0, 0, half))
            base = base + lax.rem(fine, local_rows) * op_slots
            for t in range(op_slots):
                code = code_ref[c, base + t]
                jobs[found] = (c * r_slots + j) * scale + code
                found = found + (code >= 0).astype(jnp.int32)
            return found

        return lax.fori_loop(0, r_slots, list_slot, found)

    found = lax.fori_loop(0, row_count, list_row, jnp.int32(0))
    for extra in range(BATCH):
        jobs[found + extra] = -1
    own.wait()
    near.wait()

    def batch(step, carry):
        results = []
        targets = []
        for extra in range(BATCH):
            job = jobs[step * BATCH + extra]
            valid = job >= 0
            job = jnp.maximum(job, 0)
            pair = job // scale
            code = lax.rem(job, scale)
            slot = lax.rem(code, cap)
            ahead = lax.rem(slot // own_cap + groups - group, groups)
            target = (ahead * row_count + pair // r_slots) * own_cap + lax.rem(slot, own_cap)
            targets.append(jnp.where(valid, target, last))
            results.append(
                jnp.dot(
                    r_ref[pair],
                    tiles_ref[code // cap],
                    preferred_element_type=jnp.float32,
                )
            )
        for extra in range(BATCH):
            target = targets[extra]
            out_ref[target] = out_ref[target] + results[extra]
        return carry

    lax.fori_loop(0, (found + BATCH - 1) // BATCH, batch, 0)


def sum_kernel(groups, own, part_ref, landed, send_sems, recv_sems):
    row = lax.axis_index("rows")
    group = lax.axis_index("inner")
    barrier = pltpu.get_barrier_semaphore()
    for ahead in range(1, groups):
        pl.semaphore_signal(
            barrier, inc=1, device_id=(row, lax.rem(group + ahead, groups)), device_id_type=MESH
        )
    pl.semaphore_wait(barrier, groups - 1)
    copies = []
    for ahead in range(1, groups):
        copy = pltpu.make_async_remote_copy(
            src_ref=part_ref.at[pl.ds(ahead * own, own)],
            dst_ref=landed.at[ahead - 1],
            send_sem=send_sems.at[ahead - 1],
            recv_sem=recv_sems.at[ahead - 1],
            device_id=(row, lax.rem(group + ahead, groups)),
            device_id_type=MESH,
        )
        copy.start()
        copies.append(copy)
    for copy in copies:
        copy.wait()


def sizes_for(tiles):
    steps = [16, 18, 20, 22, 24, 26, 28, 32, 40]
    return [size for size in steps if size < tiles] + [tiles]


def body(rows, groups, r_tiles, r_cols, a_tiles, a_cols, c_cols, c_counts):
    local_rows, op_slots, tile, _ = a_tiles.shape
    row_count, r_slots = r_tiles.shape[:2]
    cap = c_cols.shape[1]
    tiles = local_rows * op_slots
    half = -(-tiles // 64) * 64
    width = 2 * half
    count = rows * groups
    own_cap = cap // groups
    dims = (rows, groups, local_rows, op_slots, r_slots, cap, half)
    vmem = pl.BlockSpec(memory_space=pltpu.VMEM)
    smem = pl.BlockSpec(memory_space=pltpu.SMEM)
    anywhere = pl.BlockSpec(memory_space=pl.ANY)

    flat = a_cols.reshape(count, tiles)
    flat = jnp.pad(flat, ((0, 0), (0, half - tiles)), constant_values=-2)
    columns = jnp.concatenate([flat, flat], axis=1)

    code, plan = pl.pallas_call(
        functools.partial(plan_kernel, dims),
        out_shape=(
            jax.ShapeDtypeStruct((row_count, 2 * width), jnp.int32),
            jax.ShapeDtypeStruct((8, width), jnp.int32),
        ),
        in_specs=[vmem] * 4,
        out_specs=(vmem, vmem),
        scratch_shapes=[
            pltpu.VMEM((row_count, width), jnp.int32),
            pltpu.VMEM((count, row_count, width), jnp.int32),
            pltpu.VMEM((count, width), jnp.int32),
            pltpu.SemaphoreType.DMA,
            pltpu.SemaphoreType.DMA,
        ],
        compiler_params=pltpu.CompilerParams(collective_id=0, has_side_effects=True),
        name="plan",
    )(r_cols, c_cols, c_counts[None, :], columns)

    flat_a = a_tiles.reshape(tiles, tile, tile)
    sizes = sizes_for(tiles)

    def exchange(number, size, plan, flat_a):
        return pl.pallas_call(
            functools.partial(halo_kernel, rows, size),
            out_shape=jax.ShapeDtypeStruct((2, tiles, tile, tile), a_tiles.dtype),
            in_specs=[smem, vmem],
            out_specs=anywhere,
            scratch_shapes=[
                pltpu.VMEM((2, size, tile, tile), a_tiles.dtype),
                pltpu.SemaphoreType.DMA((2,)),
                pltpu.SemaphoreType.DMA((2,)),
            ],
            compiler_params=pltpu.CompilerParams(collective_id=number + 2, has_side_effects=True),
            name=f"halo{size}",
        )(plan, flat_a)

    level = jnp.sum((plan[3, 0] > jnp.array(sizes[:-1], jnp.int32)).astype(jnp.int32))
    halo = lax.switch(
        level,
        [functools.partial(exchange, number, size) for number, size in enumerate(sizes)],
        plan,
        flat_a,
    )

    slots = row_count * r_slots * op_slots + BATCH
    partial_value = pl.pallas_call(
        functools.partial(product_kernel, dims),
        out_shape=jax.ShapeDtypeStruct((row_count * cap + 1, tile, tile), jnp.float32),
        in_specs=[smem, smem, vmem, anywhere, anywhere],
        out_specs=vmem,
        scratch_shapes=[
            pltpu.VMEM((3 * tiles, tile, tile), a_tiles.dtype),
            pltpu.SMEM((slots,), jnp.int32),
            pltpu.SemaphoreType.DMA((2,)),
        ],
        name="products",
    )(
        code,
        r_cols,
        r_tiles.reshape(row_count * r_slots, tile, tile),
        flat_a,
        halo.reshape(2 * tiles, tile, tile),
    )

    own_count = row_count * own_cap
    landed = pl.pallas_call(
        functools.partial(sum_kernel, groups, own_count),
        out_shape=jax.ShapeDtypeStruct((groups - 1, own_count, tile, tile), jnp.float32),
        in_specs=[anywhere],
        out_specs=anywhere,
        scratch_shapes=[
            pltpu.SemaphoreType.DMA((groups - 1,)),
            pltpu.SemaphoreType.DMA((groups - 1,)),
        ],
        compiler_params=pltpu.CompilerParams(collective_id=1, has_side_effects=True),
        name="sums",
    )(partial_value)
    c_tiles = partial_value[:own_count]
    for ahead in range(groups - 1):
        c_tiles = c_tiles + landed[ahead]
    c_tiles = c_tiles.astype(jnp.bfloat16)
    return (c_tiles.reshape(row_count, own_cap, tile, tile), plan[2, :row_count])


def solution(mesh):
    rows = mesh.shape["rows"]
    groups = mesh.shape["inner"]
    return jax.shard_map(
        functools.partial(body, rows, groups),
        mesh=mesh,
        in_specs=(
            P("rows", "inner", None, None),
            P("rows", "inner"),
            P(("rows", "inner"), None, None, None),
            P(),
            P("rows", None),
            P("rows"),
        ),
        out_specs=(P("rows", "inner", None, None), P("rows")),
        check_vma=False,
    )
```

```python
import functools

import jax
import jax.numpy as jnp
from jax import lax
from jax.experimental import pallas as pl
from jax.experimental.pallas import tpu as pltpu
from jax.sharding import PartitionSpec as P

MESH = pl.DeviceIdType.MESH
BATCH = 4


def plan_kernel(
    dims, r_cols_ref, c_cols_ref, counts_ref, columns_ref, code_ref, plan_ref,
    meta_ref, gathered, needs, send_sem, recv_sem,
):
    rows, groups, local_rows, op_slots, r_slots, cap, half = dims
    width = 2 * half
    count = rows * groups
    tiles = local_rows * op_slots
    row = lax.axis_index("rows")
    group = lax.axis_index("inner")
    me = row * groups + group

    barrier = pltpu.get_barrier_semaphore()

    def place(step):
        other = lax.rem(me + step, count)
        return (other // groups, lax.rem(other, groups))

    def greet(step, carry):
        pl.semaphore_signal(barrier, inc=1, device_id=place(step), device_id_type=MESH)
        return carry

    lax.fori_loop(1, count, greet, 0)
    row_count = r_cols_ref.shape[0]
    live = r_slots + cap
    lanes = lax.broadcasted_iota(jnp.int32, (row_count, width), 1)
    above = lax.broadcasted_iota(jnp.int32, (row_count, width), 0)
    small = (row_count, row_count)
    diagonal = lax.broadcasted_iota(jnp.int32, small, 0) == lax.broadcasted_iota(jnp.int32, small, 1)
    spread_counts = jnp.broadcast_to(counts_ref[...], small)
    own_counts = jnp.sum(jnp.where(diagonal, spread_counts, 0), axis=1, keepdims=True)
    meta_ref[...] = jnp.full(meta_ref.shape, -9, jnp.int32)
    meta_ref[:, 0:r_slots] = r_cols_ref[...]
    meta_ref[:, r_slots:live] = c_cols_ref[...]
    meta_ref[:, live : live + 1] = own_counts
    gathered[me] = meta_ref[...]
    pl.semaphore_wait(barrier, count - 1)

    def post(step, carry):
        pltpu.make_async_remote_copy(
            src_ref=meta_ref,
            dst_ref=gathered.at[me],
            send_sem=send_sem,
            recv_sem=recv_sem,
            device_id=place(step),
            device_id_type=MESH,
        ).start()
        return carry

    lax.fori_loop(1, count, post, 0)
    everyone = gathered.at[pl.ds(0, count - 1)]
    pltpu.make_async_copy(everyone, everyone, send_sem).wait()
    pltpu.make_async_copy(everyone, everyone, recv_sem).wait()

    def matches(block, columns, fine_rows):
        named = fine_rows == block[:, 0:1]
        for j in range(1, r_slots):
            named = named | (fine_rows == block[:, j : j + 1])
        slot = jnp.full((row_count, width), -1, jnp.int32)
        for s in range(cap):
            slot = jnp.where(columns == block[:, r_slots + s : r_slots + s + 1], s, slot)
        return jnp.where(named, slot, -1)

    shift = jnp.where(lanes < half, -groups, groups) * local_rows
    tile = jnp.where(lanes < half, lanes, lanes - half)
    lane_rows = jnp.where(tile < tiles, shift + tile // op_slots, -(1 << 24))
    low_lanes = lanes[0:1] < half

    def near_matches(device):
        before = columns_ref[pl.ds(jnp.maximum(device - groups, 0), 1), :]
        after = columns_ref[pl.ds(jnp.minimum(device + groups, count - 1), 1), :]
        columns = jnp.where(low_lanes, before, after)
        return matches(gathered[device], columns, lane_rows + device * local_rows)

    def wanted(found):
        return jnp.max((found >= 0).astype(jnp.int32), axis=0, keepdims=True)

    def gather_needs(device, carry):
        needs[pl.ds(device, 1), :] = wanted(near_matches(device))
        return carry

    lax.fori_loop(0, count, gather_needs, 0, unroll=4)
    every = needs[...]
    low_side = lax.broadcasted_iota(jnp.int32, every.shape, 1) < half
    low = jnp.sum(jnp.where(low_side, every, 0), axis=1, keepdims=True)
    high = jnp.sum(jnp.where(low_side, 0, every), axis=1, keepdims=True)
    most = jnp.max(jnp.maximum(low, high), axis=0, keepdims=True)

    down = lax.broadcasted_iota(jnp.int32, (width, width), 0)
    across = lax.broadcasted_iota(jnp.int32, (width, width), 1)
    same = (down < half) == (across < half)

    def ranks(need):
        spread = jnp.broadcast_to(need, (width, width))
        column = jnp.sum(jnp.where(down == across, spread, 0), axis=1, keepdims=True)
        before = jnp.sum(jnp.where((across < down) & same, spread, 0), axis=1, keepdims=True)
        along = jnp.sum(
            jnp.where((down < across) & same, jnp.broadcast_to(column, (width, width)), 0),
            axis=0,
            keepdims=True,
        )
        return column, before, along

    def send_list(device, high):
        column, before, _ = ranks(needs[pl.ds(device, 1), :])
        first = half if high else 0
        mine = (down >= half) if high else (down < half)
        chosen = mine & (column > 0) & (before == across)
        return jnp.sum(jnp.where(chosen, down - first, 0), axis=0, keepdims=True)

    left = jnp.maximum(row - 1, 0) * groups + group
    right = jnp.minimum(row + 1, rows - 1) * groups + group
    plan_ref[0:1, :] = send_list(left, True)
    plan_ref[1:2, :] = send_list(right, False)

    found = near_matches(me)
    _, _, along = ranks(wanted(found))
    slot_at = along + jnp.where(lanes[0:1] < half, tiles, 2 * tiles)
    code_ref[:, 0:width] = jnp.where(found >= 0, found + cap * slot_at, -1)
    fine = me * local_rows + jnp.where(lanes < tiles, lanes // op_slots, 0)
    fine = jnp.where(lanes < tiles, fine, -5)
    found = matches(gathered[me], columns_ref[pl.ds(me, 1), :], fine)
    code_ref[:, width:] = jnp.where(found >= 0, found + cap * lanes, -1)

    def earlier(index, total):
        block = gathered[index * groups]
        return total + jnp.sum(block[:, live : live + 1], axis=0, keepdims=True)

    first = lax.fori_loop(0, row, earlier, jnp.zeros((1, 1), jnp.int32))
    counts = jnp.broadcast_to(own_counts, (row_count, width))
    inner_sum = jnp.sum(jnp.where(above < lanes, counts, 0), axis=0, keepdims=True)
    plan_ref[2:3, :] = inner_sum + first
    level = jnp.zeros((1, 1), jnp.int32)
    for size in sizes_for(tiles)[:-1]:
        level = level + (most > size).astype(jnp.int32)
    plan_ref[3:4, :] = jnp.broadcast_to(level, (1, width))


def halo_kernel(rows, size, plan_ref, a_ref, out_ref, packed, send_sems, recv_sems):
    row = lax.axis_index("rows")
    group = lax.axis_index("inner")
    barrier = pltpu.get_barrier_semaphore()
    has_left = row > 0
    has_right = row < rows - 1

    @pl.when(has_left)
    def _():
        pl.semaphore_signal(barrier, inc=1, device_id=(row - 1, group), device_id_type=MESH)

    @pl.when(has_right)
    def _():
        pl.semaphore_signal(barrier, inc=1, device_id=(row + 1, group), device_id_type=MESH)

    def pack(index, carry):
        packed[0, index] = a_ref[plan_ref[0, index]]
        packed[1, index] = a_ref[plan_ref[1, index]]
        return carry

    lax.fori_loop(0, size, pack, 0, unroll=2)

    pl.semaphore_wait(barrier, has_left.astype(jnp.int32) + has_right.astype(jnp.int32))

    def copy(side, other):
        return pltpu.make_async_remote_copy(
            src_ref=packed.at[side],
            dst_ref=out_ref.at[1 - side, pl.ds(0, size)],
            send_sem=send_sems.at[side],
            recv_sem=recv_sems.at[1 - side],
            device_id=(other, group),
            device_id_type=MESH,
        )

    @pl.when(has_left)
    def _():
        copy(0, row - 1).start()

    @pl.when(has_right)
    def _():
        copy(1, row + 1).start()

    @pl.when(has_left)
    def _():
        copy(0, row - 1).wait_send()
        copy(1, row - 1).wait_recv()

    @pl.when(has_right)
    def _():
        copy(1, row + 1).wait_send()
        copy(0, row + 1).wait_recv()


def product_kernel(dims, code_ref, cols_ref, r_ref, a_ref, halo_ref, out_ref, tiles_ref, jobs, sems):
    rows, groups, local_rows, op_slots, r_slots, cap, half = dims
    width = 2 * half
    tiles = local_rows * op_slots
    row_count = cols_ref.shape[0]
    own_cap = cap // groups
    row = lax.axis_index("rows")
    group = lax.axis_index("inner")
    own = pltpu.make_async_copy(a_ref, tiles_ref.at[pl.ds(0, tiles)], sems.at[0])
    near = pltpu.make_async_copy(halo_ref, tiles_ref.at[pl.ds(tiles, 2 * tiles)], sems.at[1])
    own.start()
    near.start()
    last = groups * row_count * own_cap
    scale = 1 << (3 * tiles * cap - 1).bit_length()

    def clear(index, carry):
        out_ref[index] = jnp.zeros(out_ref.shape[1:], jnp.float32)
        return carry

    lax.fori_loop(0, last, clear, 0, unroll=4)

    def list_row(c, found):
        def list_slot(j, found):
            fine = cols_ref[c, j]
            side = fine // (local_rows * groups) - row
            base = jnp.where(side == 0, width, jnp.where(side < 0, 0, half))
            base = base + lax.rem(fine, local_rows) * op_slots
            for t in range(op_slots):
                code = code_ref[c, base + t]
                jobs[found] = (c * r_slots + j) * scale + code
                found = found + (code >= 0).astype(jnp.int32)
            return found

        return lax.fori_loop(0, r_slots, list_slot, found)

    found = lax.fori_loop(0, row_count, list_row, jnp.int32(0))
    for extra in range(BATCH):
        jobs[found + extra] = -1
    own.wait()
    near.wait()

    def batch(step, carry):
        results = []
        targets = []
        for extra in range(BATCH):
            job = jobs[step * BATCH + extra]
            valid = job >= 0
            job = jnp.maximum(job, 0)
            pair = job // scale
            code = lax.rem(job, scale)
            slot = lax.rem(code, cap)
            ahead = lax.rem(slot // own_cap + groups - group, groups)
            target = (ahead * row_count + pair // r_slots) * own_cap + lax.rem(slot, own_cap)
            targets.append(jnp.where(valid, target, last))
            results.append(
                jnp.dot(
                    r_ref[pair],
                    tiles_ref[code // cap],
                    preferred_element_type=jnp.float32,
                )
            )
        for extra in range(BATCH):
            target = targets[extra]
            out_ref[target] = out_ref[target] + results[extra]
        return carry

    lax.fori_loop(0, (found + BATCH - 1) // BATCH, batch, 0)


def sum_kernel(groups, own, part_ref, landed, send_sems, recv_sems):
    row = lax.axis_index("rows")
    group = lax.axis_index("inner")
    barrier = pltpu.get_barrier_semaphore()
    for ahead in range(1, groups):
        pl.semaphore_signal(
            barrier, inc=1, device_id=(row, lax.rem(group + ahead, groups)), device_id_type=MESH
        )
    pl.semaphore_wait(barrier, groups - 1)
    copies = []
    for ahead in range(1, groups):
        copy = pltpu.make_async_remote_copy(
            src_ref=part_ref.at[pl.ds(ahead * own, own)],
            dst_ref=landed.at[ahead - 1],
            send_sem=send_sems.at[ahead - 1],
            recv_sem=recv_sems.at[ahead - 1],
            device_id=(row, lax.rem(group + ahead, groups)),
            device_id_type=MESH,
        )
        copy.start()
        copies.append(copy)
    for copy in copies:
        copy.wait()


def sizes_for(tiles):
    steps = [16, 18, 20, 21, 22, 23, 24, 25, 26, 27, 28, 29, 30, 32, 36, 42]
    return [size for size in steps if size < tiles] + [tiles]


def body(rows, groups, r_tiles, r_cols, a_tiles, a_cols, c_cols, c_counts):
    local_rows, op_slots, tile, _ = a_tiles.shape
    row_count, r_slots = r_tiles.shape[:2]
    cap = c_cols.shape[1]
    tiles = local_rows * op_slots
    half = -(-tiles // 64) * 64
    width = 2 * half
    count = rows * groups
    own_cap = cap // groups
    dims = (rows, groups, local_rows, op_slots, r_slots, cap, half)
    vmem = pl.BlockSpec(memory_space=pltpu.VMEM)
    smem = pl.BlockSpec(memory_space=pltpu.SMEM)
    anywhere = pl.BlockSpec(memory_space=pl.ANY)

    flat = a_cols.reshape(count, tiles)
    flat = jnp.pad(flat, ((0, 0), (0, half - tiles)), constant_values=-2)
    columns = jnp.concatenate([flat, flat], axis=1)

    code, plan = pl.pallas_call(
        functools.partial(plan_kernel, dims),
        out_shape=(
            jax.ShapeDtypeStruct((row_count, 2 * width), jnp.int32),
            jax.ShapeDtypeStruct((8, width), jnp.int32),
        ),
        in_specs=[vmem] * 4,
        out_specs=(vmem, vmem),
        scratch_shapes=[
            pltpu.VMEM((row_count, width), jnp.int32),
            pltpu.VMEM((count, row_count, width), jnp.int32),
            pltpu.VMEM((count, width), jnp.int32),
            pltpu.SemaphoreType.DMA,
            pltpu.SemaphoreType.DMA,
        ],
        compiler_params=pltpu.CompilerParams(collective_id=0, has_side_effects=True),
        name="plan",
    )(r_cols, c_cols, c_counts[None, :], columns)

    flat_a = a_tiles.reshape(tiles, tile, tile)
    sizes = sizes_for(tiles)

    def exchange(number, size, plan, flat_a):
        return pl.pallas_call(
            functools.partial(halo_kernel, rows, size),
            out_shape=jax.ShapeDtypeStruct((2, tiles, tile, tile), a_tiles.dtype),
            in_specs=[smem, vmem],
            out_specs=anywhere,
            scratch_shapes=[
                pltpu.VMEM((2, size, tile, tile), a_tiles.dtype),
                pltpu.SemaphoreType.DMA((2,)),
                pltpu.SemaphoreType.DMA((2,)),
            ],
            compiler_params=pltpu.CompilerParams(collective_id=number + 2, has_side_effects=True),
            name=f"halo{size}",
        )(plan, flat_a)

    halo = lax.switch(
        plan[3, 0],
        [functools.partial(exchange, number, size) for number, size in enumerate(sizes)],
        plan,
        flat_a,
    )

    slots = row_count * r_slots * op_slots + BATCH
    partial_value = pl.pallas_call(
        functools.partial(product_kernel, dims),
        out_shape=jax.ShapeDtypeStruct((row_count * cap + 1, tile, tile), jnp.float32),
        in_specs=[smem, smem, vmem, anywhere, anywhere],
        out_specs=vmem,
        scratch_shapes=[
            pltpu.VMEM((3 * tiles, tile, tile), a_tiles.dtype),
            pltpu.SMEM((slots,), jnp.int32),
            pltpu.SemaphoreType.DMA((2,)),
        ],
        name="products",
    )(
        code,
        r_cols,
        r_tiles.reshape(row_count * r_slots, tile, tile),
        flat_a,
        halo.reshape(2 * tiles, tile, tile),
    )

    own_count = row_count * own_cap
    landed = pl.pallas_call(
        functools.partial(sum_kernel, groups, own_count),
        out_shape=jax.ShapeDtypeStruct((groups - 1, own_count, tile, tile), jnp.float32),
        in_specs=[anywhere],
        out_specs=anywhere,
        scratch_shapes=[
            pltpu.SemaphoreType.DMA((groups - 1,)),
            pltpu.SemaphoreType.DMA((groups - 1,)),
        ],
        compiler_params=pltpu.CompilerParams(collective_id=1, has_side_effects=True),
        name="sums",
    )(partial_value)
    c_tiles = partial_value[:own_count]
    for ahead in range(groups - 1):
        c_tiles = c_tiles + landed[ahead]
    c_tiles = c_tiles.astype(jnp.bfloat16)
    return (c_tiles.reshape(row_count, own_cap, tile, tile), plan[2, :row_count])


def solution(mesh):
    rows = mesh.shape["rows"]
    groups = mesh.shape["inner"]
    return jax.shard_map(
        functools.partial(body, rows, groups),
        mesh=mesh,
        in_specs=(
            P("rows", "inner", None, None),
            P("rows", "inner"),
            P(("rows", "inner"), None, None, None),
            P(),
            P("rows", None),
            P("rows"),
        ),
        out_specs=(P("rows", "inner", None, None), P("rows")),
        check_vma=False,
    )
```
